16 devices in a mesh: dp: 2 (over y, z), sp: 8 (over x, core).
Axes of the slice: x: 4, y: 2, z: 1, core: 2. Of those that a mesh axis runs over, the one named last changes fastest.
The devices are a block of a 4x4x8 slice.
Arguments:
- q: bfloat16 [64, 32, 64], P('dp'), parts along dimension 0
- k: bfloat16 [64, 4096, 32, 64], P('dp', 'sp'), parts along dimension 0
- v: bfloat16 [64, 4096, 32, 64], P('dp', 'sp'), parts along dimension 0
Outputs:
- q: bfloat16 [64, 32, 64], P('dp'), parts along dimension 0
There are 2 independent parts. The reference program is written for one: setup_inputs(seed, part) draws one part's arguments, and reference() takes and returns one part's arrays. A program takes and returns all parts, laid end to end along the dimension named above; each array names one.
All inputs are finite; a program needn't handle non-finite values.
Results may differ from the reference program's by a relative error of at most 0.012.
Values are sent between devices in bfloat16 or wider.
A program may use at most 768 MiB of HBM per device.

```python
import jax
import jax.numpy as jnp

BATCH = 32
CACHE = 4096
HEADS = 32
KV_HEADS = 32
HEAD = 64


def setup_inputs(seed: int = 0, part: int = 0) -> dict:
    kq, kk, kv = (jax.random.fold_in(k, part) for k in jax.random.split(jax.random.key(seed), 3))
    return {
        "q": (3 * jax.random.normal(kq, (BATCH, HEADS, HEAD), jnp.float32)).astype(jnp.bfloat16),
        "k": jax.random.normal(kk, (BATCH, CACHE, KV_HEADS, HEAD), jnp.float32).astype(jnp.bfloat16),
        "v": jax.random.normal(kv, (BATCH, CACHE, KV_HEADS, HEAD), jnp.float32).astype(jnp.bfloat16),
    }


def einsum(form, a, b):
    return jnp.einsum(form, a.astype(jnp.float32), b.astype(jnp.float32))


def reference(q, k, v):
    grouped = q.reshape(BATCH, KV_HEADS, -1, HEAD)
    scores = einsum("bgsd,bugd->bgsu", grouped, k) * HEAD**-0.5
    weights = jax.nn.softmax(scores, -1).astype(jnp.bfloat16)
    return einsum("bgsu,bugd->bgsd", weights, v).astype(jnp.bfloat16).reshape(BATCH, HEADS, HEAD)
```

```python
import functools

import jax
import jax.numpy as jnp
from jax import lax
from jax.experimental import pallas as pl
from jax.experimental.pallas import tpu as pltpu
from jax.sharding import PartitionSpec as P

ROWS = 8
SLOTS = 6
ENDS = (8, 16, 24, 28, 30, 31, 32)


def kernel(n, q_hbm, k_hbm, v_hbm, o_ref, qbuf, kbuf, vbuf, wbuf, parts, stats, q_sem, k_sem, v_sem, send_sem, recv_sem):
    batch, heads, dim = q_hbm.shape
    tokens = k_hbm.shape[2]
    chunks, wide = heads // ROWS, ROWS * dim
    me = lax.axis_index("sp")
    ends = tuple(e for e in ENDS if e < batch) + (batch,)
    f32 = jnp.float32

    def fetch(hbm, buf, sem, b):
        slot = lax.rem(b, SLOTS)
        return pltpu.make_async_copy(hbm.at[b], buf.at[slot], sem.at[slot])

    q_copy = pltpu.make_async_copy(q_hbm, qbuf, q_sem)
    q_copy.start()
    for b in range(SLOTS):
        fetch(k_hbm, kbuf, k_sem, b).start()
        fetch(v_hbm, vbuf, v_sem, b).start()

    barrier = pltpu.get_barrier_semaphore()
    for j in range(1, n):
        pl.semaphore_signal(barrier, inc=1, device_id={"sp": lax.rem(me + j, n)}, device_id_type=pl.DeviceIdType.MESH)

    row = lax.broadcasted_iota(jnp.int32, (ROWS, wide), 0)
    col = lax.broadcasted_iota(jnp.int32, (ROWS, wide), 1)
    own = (col // dim) == row
    lane = lax.broadcasted_iota(jnp.int32, (ROWS, 128), 1)
    even = (lax.broadcasted_iota(jnp.int32, (ROWS, 128), 0) % 2) == 0
    first = (lane < dim) == even

    def score(b, held):
        slot = lax.rem(b, SLOTS)
        highs, totals = held
        for c in range(chunks):
            query = qbuf[b, c * ROWS : (c + 1) * ROWS, :].astype(f32)
            spread = jnp.where(own, jnp.concatenate([query] * ROWS, axis=1), 0.0).astype(jnp.bfloat16)
            s = jnp.dot(spread, kbuf[slot, c * wide : (c + 1) * wide, :], preferred_element_type=f32) * dim**-0.5
            high = jnp.max(s, -1, keepdims=True)
            w = jnp.exp(s - high)
            total = jnp.sum(w, -1, keepdims=True)
            wbuf[c] = w.astype(jnp.bfloat16)
            here = lane == b * chunks + c
            highs = jnp.where(here, high, highs)
            totals = jnp.where(here, total, totals)
        return highs, totals

    def see(b):
        slot = lax.rem(b, SLOTS)
        seen = []
        for c in range(chunks):
            r = lax.dot_general(wbuf[c], vbuf[slot, c * wide : (c + 1) * wide, :], (((1,), (1,)), ((), ())), preferred_element_type=f32)
            r = jnp.where(own, r, 0.0)
            seen.append(sum(r[:, i * 128 : (i + 1) * 128] for i in range(wide // 128)))
        pairs = [seen[c] + pltpu.roll(seen[c + 1], dim, 1) for c in range(0, chunks, 2)]
        parts[me, b] = jnp.concatenate(pairs, 0).astype(jnp.bfloat16)

    def body(t, held):
        fetch(k_hbm, kbuf, k_sem, t).wait()
        fetch(v_hbm, vbuf, v_sem, t - 1).wait()
        see(t - 1)
        held = score(t, held)

        @pl.when(t + SLOTS < batch)
        def _():
            fetch(k_hbm, kbuf, k_sem, t + SLOTS).start()

        @pl.when(t - 1 + SLOTS < batch)
        def _():
            fetch(v_hbm, vbuf, v_sem, t - 1 + SLOTS).start()

        return held

    def copies(s, lo, hi, j, source):
        to = {"sp": lax.rem(me + j, n)}
        return [
            pltpu.make_async_remote_copy(
                src_ref=ref, dst_ref=ref, send_sem=send_sem.at[s, j - 1, x], recv_sem=recv_sem.at[s, j - 1, x],
                device_id=to, device_id_type=pl.DeviceIdType.MESH,
            )
            for x, ref in enumerate((parts.at[source, pl.ds(lo, hi - lo)], stats.at[source, s]))
        ]

    def send(s, lo, hi):
        for j in range(1, n):
            for copy in copies(s, lo, hi, j, me):
                copy.start()

    def together(s, lo, hi):
        for j in range(1, n):
            for copy in copies(s, lo, hi, j, lax.rem(me + n - j, n)):
                copy.wait_recv()
        high = stats[0, s, 0]
        for i in range(1, n):
            high = jnp.maximum(high, stats[i, s, 0])
        scales = [jnp.exp(stats[i, s, 0] - high) for i in range(n)]
        total = sum(stats[i, s, 1] * scales[i] for i in range(n))
        scales = [x / total for x in scales]
        for b in range(lo, hi):
            sums = [0.0] * (chunks // 2)
            for i in range(n):
                part = parts[i, b].astype(f32)
                for p in range(chunks // 2):
                    at = b * chunks + 2 * p
                    factor = jnp.where(first, scales[i][:, at : at + 1], scales[i][:, at + 1 : at + 2])
                    sums[p] += part[p * ROWS : (p + 1) * ROWS] * factor
            out = []
            for x in sums:
                y = pltpu.roll(x, dim, 1)
                out += [jnp.where(even, x, y)[:, :dim], jnp.where(even, y, x)[:, :dim]]
            o_ref[b] = jnp.concatenate(out, 0).astype(o_ref.dtype)

    q_copy.wait()
    fetch(k_hbm, kbuf, k_sem, 0).wait()
    zero = jnp.zeros((ROWS, 128), f32)
    held = score(0, (zero, zero))
    fetch(k_hbm, kbuf, k_sem, SLOTS).start()
    lo = 0
    done = []
    for s, hi in enumerate(ends):
        if hi < batch:
            held = lax.fori_loop(lo + 1, hi + 1, body, held)
        else:
            held = lax.fori_loop(lo + 1, hi, body, held)
            fetch(v_hbm, vbuf, v_sem, batch - 1).wait()
            see(batch - 1)
        stats[me, s, 0], stats[me, s, 1] = held
        if s == 0:
            pl.semaphore_wait(barrier, n - 1)
        send(s, lo, hi)
        done.append((s, lo, hi))
        if s >= 1 and s < len(ends) - 1:
            together(*done[s - 1])
        lo = hi
    for seg in done[-2:]:
        together(*seg)
    for s, lo, hi in done:
        for j in range(1, n):
            for copy in copies(s, lo, hi, j, me):
                copy.wait_send()


def solution(mesh):
    n = mesh.shape["sp"]

    def step(q, k, v):
        batch, tokens, heads, dim = k.shape
        k, v = (x.transpose(0, 2, 3, 1).reshape(batch, heads * dim, tokens) for x in (k, v))
        segments = len([e for e in ENDS if e < batch]) + 1
        hbm = pl.BlockSpec(memory_space=pltpu.HBM)
        return pl.pallas_call(
            functools.partial(kernel, n),
            out_shape=jax.ShapeDtypeStruct(q.shape, q.dtype),
            in_specs=[hbm] * 3,
            out_specs=pl.BlockSpec(memory_space=pltpu.VMEM),
            scratch_shapes=[
                pltpu.VMEM(q.shape, q.dtype),
                pltpu.VMEM((SLOTS, heads * dim, tokens), k.dtype),
                pltpu.VMEM((SLOTS, heads * dim, tokens), v.dtype),
                pltpu.VMEM((heads // ROWS, ROWS, tokens), jnp.bfloat16),
                pltpu.VMEM((n, batch, heads // 2, 2 * dim), jnp.bfloat16),
                pltpu.VMEM((n, segments, 2, ROWS, 128), jnp.float32),
                pltpu.SemaphoreType.DMA,
                pltpu.SemaphoreType.DMA((SLOTS,)),
                pltpu.SemaphoreType.DMA((SLOTS,)),
                pltpu.SemaphoreType.DMA((segments, n - 1, 2)),
                pltpu.SemaphoreType.DMA((segments, n - 1, 2)),
            ],
            compiler_params=pltpu.CompilerParams(collective_id=0, has_side_effects=True, vmem_limit_bytes=40 * 2**20),
            cost_estimate=pl.CostEstimate(flops=4 * k.size, bytes_accessed=4 * k.size, transcendentals=batch * heads * tokens),
        )(q, k, v)

    return jax.shard_map(
        step,
        mesh=mesh,
        in_specs=(P("dp", None, None), P("dp", "sp", None, None), P("dp", "sp", None, None)),
        out_specs=P("dp", None, None),
        check_vma=False,
    )
```

```python
import functools

import jax
import jax.numpy as jnp
from jax import lax
from jax.experimental import pallas as pl
from jax.experimental.pallas import tpu as pltpu
from jax.sharding import PartitionSpec as P

ROWS = 8
SLOTS = 6
LEAD = 8
SOME = 4
TAIL = 4
PEERS = pl.DeviceIdType.MESH


def spans(batch, ends):
    ends = tuple(range(SOME, batch - TAIL + 1, SOME)) + tuple(batch - TAIL + e for e in ends)
    return tuple(zip((0,) + ends[:-1], ends))


def kernel(n, q_hbm, k_hbm, v_hbm, o_ref, qbuf, kbuf, vbuf, wbuf, parts, stats, share, *sems):
    q_sem, k_sem, v_sem, tail_sem, go_sem, came_sem, out_sem, in_sem = sems
    batch, heads, dim = q_hbm.shape
    chunks, wide = heads // ROWS, ROWS * dim
    last = batch - 1
    me = lax.axis_index("sp")
    f32 = jnp.float32
    runs, segments = spans(batch, (2, 4)), spans(batch, (2, 3, 4))
    many = (batch - TAIL) // SOME

    def fetch(hbm, buf, sem, b):
        slot = lax.rem(b, SLOTS)
        return pltpu.make_async_copy(hbm.at[b], buf.at[slot], sem.at[slot])

    def piece(c):
        rows = pl.ds(c * wide, wide)
        return pltpu.make_async_copy(v_hbm.at[last, rows], vbuf.at[last % SLOTS, rows], tail_sem.at[c])

    def more(t):
        @pl.when(t + SLOTS < batch)
        def _():
            fetch(k_hbm, kbuf, k_sem, t + SLOTS).start(priority=1)

        @pl.when(jnp.logical_and(t - LEAD + SLOTS >= 0, t - LEAD + SLOTS < last))
        def _():
            fetch(v_hbm, vbuf, v_sem, t - LEAD + SLOTS).start(priority=1)

        @pl.when(t - LEAD + SLOTS == last)
        def _():
            for c in range(chunks):
                piece(c).start(priority=1)

    q_copy = pltpu.make_async_copy(q_hbm, qbuf, q_sem)
    q_copy.start()
    for b in range(SLOTS):
        fetch(k_hbm, kbuf, k_sem, b).start(priority=1)
        if b >= LEAD:
            fetch(v_hbm, vbuf, v_sem, b - LEAD).start(priority=1)

    barrier = pltpu.get_barrier_semaphore()
    for j in range(1, n):
        pl.semaphore_signal(barrier, inc=1, device_id={"sp": lax.rem(me + j, n)}, device_id_type=PEERS)

    row = lax.broadcasted_iota(jnp.int32, (ROWS, wide), 0)
    block = lax.broadcasted_iota(jnp.int32, (ROWS, wide), 1) // dim
    own = [block == row, block == row + 1 - 2 * (row % 2)]
    head = lax.broadcasted_iota(jnp.int32, (ROWS, 128), 0)
    lane = lax.broadcasted_iota(jnp.int32, (ROWS, 128), 1)
    even = (head % 2) == 0

    def run_of(b):
        return jnp.where(b < batch - TAIL, lax.div(b, SOME), many + lax.div(b - (batch - TAIL), 2))

    def place(b, c):
        return lax.rem(b, SOME) * chunks + c

    def swap(x):
        odd = lax.broadcasted_iota(jnp.int32, x.shape, 0) % 2
        return jnp.where(odd == 0, pltpu.roll(x, ROWS - 1, 0), pltpu.roll(x, 1, 0))

    def score(b):
        slot, g = lax.rem(b, SLOTS), run_of(b)
        line = jnp.where(lax.rem(b, SOME) == 0, 0.0, stats[me, g])
        for c in range(chunks):
            query = qbuf[b, c * ROWS : (c + 1) * ROWS, :].astype(f32)
            if c % 2:
                query = swap(query)
            spread = jnp.where(own[c % 2], jnp.concatenate([query] * ROWS, axis=1), 0.0).astype(jnp.bfloat16)
            s = jnp.dot(spread, kbuf[slot, c * wide : (c + 1) * wide, :], preferred_element_type=f32) * dim**-0.5
            high = jnp.max(s, -1, keepdims=True)
            w = jnp.exp(s - high)
            wbuf[lax.rem(b, LEAD + 1), c] = w.astype(jnp.bfloat16)
            line = jnp.where(lane == place(b, c), high, line)
            line = jnp.where(lane == 64 + place(b, c), jnp.sum(w, -1, keepdims=True), line)
        stats[me, g] = line

    def weights(b):
        return [wbuf[lax.rem(b, LEAD + 1), c] for c in range(chunks)]

    def see(b, weight, ready=lambda c: None):
        slot = lax.rem(b, SLOTS)
        shares = share[...]
        seen = []
        for c in range(chunks):
            ready(c)
            mine = jnp.sum(jnp.where(lane == place(b, c), shares, 0.0), -1, keepdims=True)
            r = lax.dot_general(weight[c], vbuf[slot, c * wide : (c + 1) * wide, :], (((1,), (1,)), ((), ())), preferred_element_type=f32)
            r = jnp.where(own[c % 2], r, 0.0)
            seen.append(sum(r[:, i * 128 : (i + 1) * 128] for i in range(wide // 128)) * mine)
        pairs = [seen[c] + seen[c + 1] for c in range(0, chunks, 2)]
        parts[me, b] = jnp.concatenate(pairs, 0).astype(jnp.bfloat16)

    def remote(ref, out, came, to):
        return pltpu.make_async_remote_copy(src_ref=ref, dst_ref=ref, send_sem=out, recv_sem=came, device_id={"sp": to}, device_id_type=PEERS)

    def ahead(j):
        return lax.rem(me + j, n)

    def behind(j):
        return lax.rem(me + n - j, n)

    def line_to(g, j, source):
        return remote(stats.at[source, g], go_sem.at[g, j - 1], came_sem.at[g, j - 1], ahead(j))

    def part_to(s, lo, size, j, source):
        return remote(parts.at[source, pl.ds(lo, size)], out_sem.at[s, j - 1], in_sem.at[s, j - 1], ahead(j))

    def send_lines(g):
        for j in range(1, n):
            line_to(g, j, me).start()

    def send_parts(s, lo, size):
        for j in range(1, n):
            part_to(s, lo, size, j, me).start()

    def weigh(g):
        for j in range(1, n):
            line_to(g, j, behind(j)).wait_recv()
        high = functools.reduce(jnp.maximum, [stats[i, g] for i in range(n)])
        total = sum(pltpu.roll(stats[i, g], 64, 1) * jnp.exp(stats[i, g] - high) for i in range(n))
        share[...] = jnp.exp(stats[me, g] - high) / total

    def scored(t):
        whole = jnp.logical_and(lax.rem(t, SOME) == SOME - 1, t < batch - TAIL)
        pl.when(whole)(lambda: send_lines(lax.div(t, SOME)))
        for g, (lo, hi) in list(enumerate(runs))[many:]:
            pl.when(t == hi - 1)(functools.partial(send_lines, g))

    def first_of(b):
        whole = jnp.logical_and(lax.rem(b, SOME) == 0, b < batch - TAIL)
        pl.when(whole)(lambda: weigh(lax.div(b, SOME)))

    def seen_all(b):
        whole = jnp.logical_and(lax.rem(b, SOME) == SOME - 1, b < batch - TAIL)
        pl.when(whole)(lambda: send_parts(lax.div(b, SOME), b - (SOME - 1), SOME))

    def body(t, nothing):
        f = t - LEAD
        first_of(f)
        fetch(k_hbm, kbuf, k_sem, t).wait()
        fetch(v_hbm, vbuf, v_sem, f).wait()
        held = weights(f)
        score(t)
        see(f, held)
        more(t)
        scored(t)
        seen_all(f)
        return nothing

    q_copy.wait()
    for t in range(LEAD):
        fetch(k_hbm, kbuf, k_sem, t).wait()
        score(jnp.int32(t))
        more(jnp.int32(t))
        if t == SOME - 1:
            pl.semaphore_wait(barrier, n - 1)
        if t % SOME == SOME - 1:
            send_lines(t // SOME)
    lax.fori_loop(LEAD, batch, body, 0)
    b = batch - LEAD
    while b < batch:
        size = 2 if b + 2 < last else 1
        for x in range(b, b + size):
            for g, (lo, hi) in enumerate(runs):
                if lo == x:
                    weigh(g)
            if x < last:
                fetch(v_hbm, vbuf, v_sem, x).wait()
        for x in range(b, b + size):
            see(x, weights(x), (lambda c: piece(c).wait()) if x == last else (lambda c: None))
        for x in range(b, b + size):
            more(jnp.int32(x + LEAD))
        for x in range(b, b + size):
            for s, (lo, hi) in enumerate(segments):
                if hi - 1 == x:
                    send_parts(s, lo, hi - lo)
        b += size

    for s, (lo, hi) in enumerate(segments):
        for j in range(1, n):
            part_to(s, lo, hi - lo, j, behind(j)).wait_recv()
        for b in range(lo, hi):
            x = sum(parts[i, b].astype(f32) for i in range(n))
            out = []
            for p in range(chunks // 2):
                y = x[p * ROWS : (p + 1) * ROWS]
                z = pltpu.roll(y, dim, 1)
                out += [jnp.where(even, y, z)[:, :dim], swap(jnp.where(even, z, y))[:, :dim]]
            o_ref[b] = jnp.concatenate(out, 0).astype(o_ref.dtype)
    for j in range(1, n):
        for g in range(len(runs)):
            line_to(g, j, me).wait_send()
        for s, (lo, hi) in enumerate(segments):
            part_to(s, lo, hi - lo, j, me).wait_send()


def solution(mesh):
    n = mesh.shape["sp"]

    def step(q, k, v):
        batch, tokens, heads, dim = k.shape
        k, v = (x.transpose(0, 2, 3, 1).reshape(batch, heads * dim, tokens) for x in (k, v))
        chunks = heads // ROWS
        runs, segments = len(spans(batch, (2, 4))), len(spans(batch, (2, 3, 4)))
        hbm = pl.BlockSpec(memory_space=pl.ANY)
        dma = pltpu.SemaphoreType.DMA
        return pl.pallas_call(
            functools.partial(kernel, n),
            out_shape=jax.ShapeDtypeStruct(q.shape, q.dtype),
            in_specs=[hbm] * 3,
            out_specs=pl.BlockSpec(memory_space=pltpu.VMEM),
            scratch_shapes=[
                pltpu.VMEM(q.shape, q.dtype),
                pltpu.VMEM((SLOTS, heads * dim, tokens), k.dtype),
                pltpu.VMEM((SLOTS, heads * dim, tokens), v.dtype),
                pltpu.VMEM((LEAD + 1, chunks, ROWS, tokens), jnp.bfloat16),
                pltpu.VMEM((n, batch, heads // 2, 2 * dim), jnp.bfloat16),
                pltpu.VMEM((n, runs, ROWS, 128), jnp.float32),
                pltpu.VMEM((ROWS, 128), jnp.float32),
                dma,
                dma((SLOTS,)),
                dma((SLOTS,)),
                dma((chunks,)),
                dma((runs, n - 1)),
                dma((runs, n - 1)),
                dma((segments, n - 1)),
                dma((segments, n - 1)),
            ],
            compiler_params=pltpu.CompilerParams(collective_id=0, has_side_effects=True, vmem_limit_bytes=56114023),
            cost_estimate=pl.CostEstimate(flops=4 * k.size, bytes_accessed=4 * k.size, transcendentals=batch * heads * tokens),
        )(q, k, v)

    return jax.shard_map(
        step,
        mesh=mesh,
        in_specs=(P("dp", None, None), P("dp", "sp", None, None), P("dp", "sp", None, None)),
        out_specs=P("dp", None, None),
        check_vma=False,
    )
```

```python
import functools

import jax
import jax.numpy as jnp
from jax import lax
from jax.experimental import pallas as pl
from jax.experimental.pallas import tpu as pltpu
from jax.sharding import PartitionSpec as P

ROWS = 8
SLOTS = 6
LEAD = 8
SOME = 4
TAIL = 4
STEPS = (2, 2, 2, 1, 1)
PEERS = pl.DeviceIdType.MESH


def spans(batch, ends):
    ends = tuple(range(SOME, batch - TAIL + 1, SOME)) + tuple(batch - TAIL + e for e in ends)
    return tuple(zip((0,) + ends[:-1], ends))


def kernel(n, q_hbm, k_hbm, v_hbm, o_ref, qbuf, kbuf, vbuf, wbuf, parts, stats, share, *sems):
    q_sem, k_sem, v_sem, go_sem, came_sem, out_sem, in_sem = sems
    batch, heads, dim = q_hbm.shape
    chunks, wide = heads // ROWS, ROWS * dim
    last = batch - 1
    me = lax.axis_index("sp")
    f32 = jnp.float32
    runs, segments = spans(batch, (2, 4)), spans(batch, (2, 3, 4))
    order = sorted(range(1, n), key=lambda j: abs(j - n // 2))
    many = (batch - TAIL) // SOME

    def fetch(hbm, buf, sem, b):
        slot = lax.rem(b, SLOTS)
        return pltpu.make_async_copy(hbm.at[b], buf.at[slot], sem.at[slot])

    def more(t):
        @pl.when(t + SLOTS < batch)
        def _():
            fetch(k_hbm, kbuf, k_sem, t + SLOTS).start(priority=1)

        @pl.when(jnp.logical_and(t - LEAD + SLOTS >= 0, t - LEAD + SLOTS < batch))
        def _():
            fetch(v_hbm, vbuf, v_sem, t - LEAD + SLOTS).start(priority=1)

    q_copy = pltpu.make_async_copy(q_hbm, qbuf, q_sem)
    q_copy.start()
    for b in range(SLOTS):
        fetch(k_hbm, kbuf, k_sem, b).start(priority=1)
        if b >= LEAD:
            fetch(v_hbm, vbuf, v_sem, b - LEAD).start(priority=1)

    barrier = pltpu.get_barrier_semaphore()
    for j in range(1, n):
        pl.semaphore_signal(barrier, inc=1, device_id={"sp": lax.rem(me + j, n)}, device_id_type=PEERS)

    row = lax.broadcasted_iota(jnp.int32, (ROWS, wide), 0)
    block = lax.broadcasted_iota(jnp.int32, (ROWS, wide), 1) // dim
    own = [block == row, block == row + 1 - 2 * (row % 2)]
    head = lax.broadcasted_iota(jnp.int32, (ROWS, 128), 0)
    lane = lax.broadcasted_iota(jnp.int32, (ROWS, 128), 1)
    even = (head % 2) == 0

    def run_of(b):
        return jnp.where(b < batch - TAIL, lax.div(b, SOME), many + lax.div(b - (batch - TAIL), 2))

    def place(b, c):
        return lax.rem(b, SOME) * chunks + c

    def swap(x):
        odd = lax.broadcasted_iota(jnp.int32, x.shape, 0) % 2
        return jnp.where(odd == 0, pltpu.roll(x, ROWS - 1, 0), pltpu.roll(x, 1, 0))

    def score(b):
        slot, g = lax.rem(b, SLOTS), run_of(b)
        line = jnp.where(lax.rem(b, SOME) == 0, 0.0, stats[me, g])
        for c in range(chunks):
            query = qbuf[b, c * ROWS : (c + 1) * ROWS, :].astype(f32)
            if c % 2:
                query = swap(query)
            spread = jnp.where(own[c % 2], jnp.concatenate([query] * ROWS, axis=1), 0.0).astype(jnp.bfloat16)
            s = jnp.dot(spread, kbuf[slot, c * wide : (c + 1) * wide, :], preferred_element_type=f32) * dim**-0.5
            high = jnp.max(s, -1, keepdims=True)
            w = jnp.exp(s - high)
            wbuf[lax.rem(b, LEAD + 1), c] = w.astype(jnp.bfloat16)
            line = jnp.where(lane == place(b, c), high, line)
            line = jnp.where(lane == 64 + place(b, c), jnp.sum(w, -1, keepdims=True), line)
        stats[me, g] = line

    def weights(b):
        return [wbuf[lax.rem(b, LEAD + 1), c] for c in range(chunks)]

    def see(b, weight):
        slot = lax.rem(b, SLOTS)
        shares = share[...]
        seen = []
        for c in range(chunks):
            mine = jnp.sum(jnp.where(lane == place(b, c), shares, 0.0), -1, keepdims=True)
            r = lax.dot_general(weight[c], vbuf[slot, c * wide : (c + 1) * wide, :], (((1,), (1,)), ((), ())), preferred_element_type=f32)
            r = jnp.where(own[c % 2], r, 0.0)
            seen.append(sum(r[:, i * 128 : (i + 1) * 128] for i in range(wide // 128)) * mine)
        pairs = [seen[c] + seen[c + 1] for c in range(0, chunks, 2)]
        parts[me, b] = jnp.concatenate(pairs, 0).astype(jnp.bfloat16)

    def remote(ref, out, came, to):
        return pltpu.make_async_remote_copy(src_ref=ref, dst_ref=ref, send_sem=out, recv_sem=came, device_id={"sp": to}, device_id_type=PEERS)

    def ahead(j):
        return lax.rem(me + j, n)

    def line_to(g, j):
        return remote(stats.at[me, g], go_sem, came_sem.at[g], ahead(j))

    def part_to(x, lo, size, j):
        return remote(parts.at[me, pl.ds(lo, size)], out_sem, in_sem.at[x], ahead(j))

    def all_but_one(ref, out, came):
        return remote(ref, out, came, ahead(1))

    def send_lines(g):
        for j in order:
            line_to(g, j).start()

    def send_parts(x, lo, size):
        for j in order:
            part_to(x, lo, size, j).start()

    def weigh(g):
        all_but_one(stats.at[pl.ds(0, n - 1), g], go_sem, came_sem.at[g]).wait_recv()
        high = functools.reduce(jnp.maximum, [stats[i, g] for i in range(n)])
        total = sum(pltpu.roll(stats[i, g], 64, 1) * jnp.exp(stats[i, g] - high) for i in range(n))
        share[...] = jnp.exp(stats[me, g] - high) / total

    def scored(t):
        whole = jnp.logical_and(lax.rem(t, SOME) == SOME - 1, t < batch - TAIL)
        pl.when(whole)(lambda: send_lines(lax.div(t, SOME)))
        for g, (lo, hi) in list(enumerate(runs))[many:]:
            pl.when(t == hi - 1)(functools.partial(send_lines, g))

    def first_of(b):
        whole = jnp.logical_and(lax.rem(b, SOME) == 0, b < batch - TAIL)
        pl.when(whole)(lambda: weigh(lax.div(b, SOME)))

    def seen_all(b):
        whole = jnp.logical_and(lax.rem(b, SOME) == SOME - 1, b < batch - TAIL)
        pl.when(whole)(lambda: send_parts(0, b - (SOME - 1), SOME))

    def body(t, nothing):
        f = t - LEAD
        first_of(f)
        fetch(k_hbm, kbuf, k_sem, t).wait()
        fetch(v_hbm, vbuf, v_sem, f).wait()
        held = weights(f)
        score(t)
        see(f, held)
        more(t)
        scored(t)
        seen_all(f)
        return nothing

    q_copy.wait()
    for t in range(LEAD):
        fetch(k_hbm, kbuf, k_sem, t).wait()
        score(jnp.int32(t))
        more(jnp.int32(t))
        if t == SOME - 1:
            pl.semaphore_wait(barrier, n - 1)
        if t % SOME == SOME - 1:
            send_lines(t // SOME)
    lax.fori_loop(LEAD, batch, body, 0)
    b = batch - LEAD
    for size in STEPS:
        for x in range(b, b + size):
            for g, (lo, hi) in enumerate(runs):
                if lo == x:
                    weigh(g)
            fetch(v_hbm, vbuf, v_sem, x).wait()
        for x in range(b, b + size):
            see(x, weights(x))
        for x in range(b, b + size):
            more(jnp.int32(x + LEAD))
        for x in range(b, b + size):
            for lo, hi in segments:
                if hi - 1 == x:
                    send_parts(max(0, segments.index((lo, hi)) - many + 1), lo, hi - lo)
        b += size

    for x, (lo, hi) in enumerate(((0, batch - TAIL),) + segments[many:]):
        if hi == batch:
            all_but_one(stats.at[pl.ds(0, n - 1)], go_sem, came_sem.at[0]).wait_send()
        all_but_one(parts.at[pl.ds(0, n - 1), pl.ds(lo, hi - lo)], out_sem, in_sem.at[x]).wait_recv()
        for b in range(lo, hi):
            x = sum(parts[i, b].astype(f32) for i in range(n))
            out = []
            for p in range(chunks // 2):
                y = x[p * ROWS : (p + 1) * ROWS]
                z = pltpu.roll(y, dim, 1)
                out += [jnp.where(even, y, z)[:, :dim], swap(jnp.where(even, z, y))[:, :dim]]
            o_ref[b] = jnp.concatenate(out, 0).astype(o_ref.dtype)
    all_but_one(parts.at[pl.ds(0, n - 1)], out_sem, in_sem.at[0]).wait_send()


def solution(mesh):
    n = mesh.shape["sp"]

    def step(q, k, v):
        batch, tokens, heads, dim = k.shape
        k, v = (x.transpose(0, 2, 3, 1).reshape(batch, heads * dim, tokens) for x in (k, v))
        chunks = heads // ROWS
        runs, segments = len(spans(batch, (2, 4))), len(spans(batch, (2, 3, 4)))
        hbm = pl.BlockSpec(memory_space=pl.ANY)
        dma = pltpu.SemaphoreType.DMA
        return pl.pallas_call(
            functools.partial(kernel, n),
            out_shape=jax.ShapeDtypeStruct(q.shape, q.dtype),
            in_specs=[hbm] * 3,
            out_specs=pl.BlockSpec(memory_space=pltpu.VMEM),
            scratch_shapes=[
                pltpu.VMEM(q.shape, q.dtype),
                pltpu.VMEM((SLOTS, heads * dim, tokens), k.dtype),
                pltpu.VMEM((SLOTS, heads * dim, tokens), v.dtype),
                pltpu.VMEM((LEAD + 1, chunks, ROWS, tokens), jnp.bfloat16),
                pltpu.VMEM((n, batch, heads // 2, 2 * dim), jnp.bfloat16),
                pltpu.VMEM((n, runs, ROWS, 128), jnp.float32),
                pltpu.VMEM((ROWS, 128), jnp.float32),
                dma,
                dma((SLOTS,)),
                dma((SLOTS,)),
                dma,
                dma((runs,)),
                dma,
                dma((segments - (batch - TAIL) // SOME + 1,)),
            ],
            compiler_params=pltpu.CompilerParams(collective_id=0, has_side_effects=True, vmem_limit_bytes=56114023),
            cost_estimate=pl.CostEstimate(flops=4 * k.size, bytes_accessed=4 * k.size, transcendentals=batch * heads * tokens),
        )(q, k, v)

    return jax.shard_map(
        step,
        mesh=mesh,
        in_specs=(P("dp", None, None), P("dp", "sp", None, None), P("dp", "sp", None, None)),
        out_specs=P("dp", None, None),
        check_vma=False,
    )
```

```python
import functools

import jax
import jax.numpy as jnp
from jax import lax
from jax.experimental import pallas as pl
from jax.experimental.pallas import tpu as pltpu
from jax.sharding import PartitionSpec as P

ROWS = 8
SLOTS = 6
LEAD = 8
SOME = 4
TAIL = 4
STEPS = (2, 2, 2, 1, 1)
PEERS = pl.DeviceIdType.MESH


def spans(batch, ends):
    ends = tuple(range(SOME, batch - TAIL + 1, SOME)) + tuple(batch - TAIL + e for e in ends)
    return tuple(zip((0,) + ends[:-1], ends))


def kernel(n, q_hbm, k_hbm, v_hbm, o_ref, qbuf, kbuf, vbuf, wbuf, parts, stats, share, *sems):
    q_sem, k_sem, v_sem, go_sem, came_sem, out_sem, in_sem = sems
    batch, heads, dim = q_hbm.shape
    chunks, wide = heads // ROWS, ROWS * dim
    last = batch - 1
    me = lax.axis_index("sp")
    f32 = jnp.float32
    runs, segments = spans(batch, (2, 4)), spans(batch, (2, 3, 4))
    order = sorted(range(1, n), key=lambda j: abs(j - n // 2))
    many = (batch - TAIL) // SOME

    def fetch(hbm, buf, sem, b):
        slot = lax.rem(b, SLOTS)
        return pltpu.make_async_copy(hbm.at[b], buf.at[slot], sem.at[slot])

    def more(t):
        @pl.when(t + SLOTS < batch)
        def _():
            fetch(k_hbm, kbuf, k_sem, t + SLOTS).start(priority=1)

        @pl.when(jnp.logical_and(t - LEAD + SLOTS >= 0, t - LEAD + SLOTS < batch))
        def _():
            fetch(v_hbm, vbuf, v_sem, t - LEAD + SLOTS).start(priority=1)

    q_copy = pltpu.make_async_copy(q_hbm, qbuf, q_sem)
    q_copy.start()
    for b in range(SLOTS):
        fetch(k_hbm, kbuf, k_sem, b).start(priority=1)
        if b >= LEAD:
            fetch(v_hbm, vbuf, v_sem, b - LEAD).start(priority=1)

    barrier = pltpu.get_barrier_semaphore()
    for j in range(1, n):
        pl.semaphore_signal(barrier, inc=1, device_id={"sp": lax.rem(me + j, n)}, device_id_type=PEERS)

    row = lax.broadcasted_iota(jnp.int32, (ROWS, wide), 0)
    block = lax.broadcasted_iota(jnp.int32, (ROWS, wide), 1) // dim
    own = [block == row, block == row + 1 - 2 * (row % 2)]
    head = lax.broadcasted_iota(jnp.int32, (ROWS, 128), 0)
    lane = lax.broadcasted_iota(jnp.int32, (ROWS, 128), 1)
    even = (head % 2) == 0

    def run_of(b):
        return jnp.where(b < batch - TAIL, lax.div(b, SOME), many + lax.div(b - (batch - TAIL), 2))

    def place(b, c):
        return lax.rem(b, SOME) * chunks + c

    def swap(x):
        odd = lax.broadcasted_iota(jnp.int32, x.shape, 0) % 2
        return jnp.where(odd == 0, pltpu.roll(x, ROWS - 1, 0), pltpu.roll(x, 1, 0))

    def score(b):
        slot, g = lax.rem(b, SLOTS), run_of(b)
        line = jnp.where(lax.rem(b, SOME) == 0, 0.0, stats[me, g])
        for c in range(chunks):
            query = qbuf[b, c * ROWS : (c + 1) * ROWS, :].astype(f32)
            if c % 2:
                query = swap(query)
            spread = jnp.where(own[c % 2], jnp.concatenate([query] * ROWS, axis=1), 0.0).astype(jnp.bfloat16)
            s = jnp.dot(spread, kbuf[slot, c * wide : (c + 1) * wide, :], preferred_element_type=f32) * dim**-0.5
            high = jnp.max(s, -1, keepdims=True)
            w = jnp.exp(s - high)
            wbuf[lax.rem(b, LEAD + 1), c] = w.astype(jnp.bfloat16)
            line = jnp.where(lane == place(b, c), high, line)
            line = jnp.where(lane == 64 + place(b, c), jnp.sum(w, -1, keepdims=True), line)
        stats[me, g] = line

    def weights(b):
        return [wbuf[lax.rem(b, LEAD + 1), c] for c in range(chunks)]

    def see(b, weight):
        slot = lax.rem(b, SLOTS)
        shares = share[...]
        seen = []
        for c in range(chunks):
            mine = jnp.sum(jnp.where(lane == place(b, c), shares, 0.0), -1, keepdims=True)
            r = lax.dot_general(weight[c], vbuf[slot, c * wide : (c + 1) * wide, :], (((1,), (1,)), ((), ())), preferred_element_type=f32)
            r = jnp.where(own[c % 2], r, 0.0)
            seen.append(sum(r[:, i * 128 : (i + 1) * 128] for i in range(wide // 128)) * mine)
        pairs = [seen[c] + seen[c + 1] for c in range(0, chunks, 2)]
        parts[me, b] = jnp.concatenate(pairs, 0).astype(jnp.bfloat16)

    def remote(ref, out, came, to):
        return pltpu.make_async_remote_copy(src_ref=ref, dst_ref=ref, send_sem=out, recv_sem=came, device_id={"sp": to}, device_id_type=PEERS)

    def ahead(j):
        return lax.rem(me + j, n)

    def line_to(g, j):
        return remote(stats.at[me, g], go_sem, came_sem.at[g], ahead(j))

    def part_to(x, lo, size, j):
        return remote(parts.at[me, pl.ds(lo, size)], out_sem, in_sem.at[x], ahead(j))

    def all_but_one(ref, out, came):
        return remote(ref, out, came, ahead(1))

    def send_lines(g):
        for j in order:
            line_to(g, j).start()

    def send_parts(x, lo, size):
        for j in order:
            part_to(x, lo, size, j).start()

    def lines_in(g):
        all_but_one(stats.at[pl.ds(0, n - 1), g], go_sem, came_sem.at[g]).wait_recv()

    def weigh(g):
        high = functools.reduce(jnp.maximum, [stats[i, g] for i in range(n)])
        total = sum(pltpu.roll(stats[i, g], 64, 1) * jnp.exp(stats[i, g] - high) for i in range(n))
        share[...] = jnp.exp(stats[me, g] - high) / total

    def scored(t):
        whole = jnp.logical_and(lax.rem(t, SOME) == SOME - 1, t < batch - TAIL)
        pl.when(whole)(lambda: send_lines(lax.div(t, SOME)))
        for g, (lo, hi) in list(enumerate(runs))[many:]:
            pl.when(t == hi - 1)(functools.partial(send_lines, g))

    def first_of(b):
        whole = jnp.logical_and(lax.rem(b, SOME) == 0, b < batch - TAIL)

        @pl.when(whole)
        def _():
            lines_in(lax.div(b, SOME))
            weigh(lax.div(b, SOME))


    def seen_all(b):
        whole = jnp.logical_and(lax.rem(b, SOME) == SOME - 1, b < batch - TAIL)
        pl.when(whole)(lambda: send_parts(0, b - (SOME - 1), SOME))

    def body(t, nothing):
        f = t - LEAD
        first_of(f)
        fetch(k_hbm, kbuf, k_sem, t).wait()
        fetch(v_hbm, vbuf, v_sem, f).wait()
        held = weights(f)
        score(t)
        see(f, held)
        more(t)
        scored(t)
        seen_all(f)
        return nothing

    q_copy.wait()
    for t in range(LEAD):
        fetch(k_hbm, kbuf, k_sem, t).wait()
        score(jnp.int32(t))
        more(jnp.int32(t))
        if t == SOME - 1:
            pl.semaphore_wait(barrier, n - 1)
        if t % SOME == SOME - 1:
            send_lines(t // SOME)
    lax.fori_loop(LEAD, batch, body, 0)
    b = batch - LEAD
    due = []
    for size in STEPS:
        new = [g for g, (lo, hi) in enumerate(runs) if lo == b]
        for g in new:
            lines_in(g)
        for x in range(b, b + size):
            fetch(v_hbm, vbuf, v_sem, x).wait()
        for one in due:
            send_parts(*one)
        for g in new:
            weigh(g)
        for x in range(b, b + size):
            see(x, weights(x))
        for x in range(b, b + size):
            more(jnp.int32(x + LEAD))
        b += size
        due = [(max(0, i - many + 1), lo, hi - lo) for i, (lo, hi) in enumerate(segments) if b - size < hi <= b]
    for one in due:
        send_parts(*one)

    for x, (lo, hi) in enumerate(((0, batch - TAIL),) + segments[many:]):
        if hi == batch:
            all_but_one(stats.at[pl.ds(0, n - 1)], go_sem, came_sem.at[0]).wait_send()
        all_but_one(parts.at[pl.ds(0, n - 1), pl.ds(lo, hi - lo)], out_sem, in_sem.at[x]).wait_recv()
        for b in range(lo, hi):
            x = sum(parts[i, b].astype(f32) for i in range(n))
            out = []
            for p in range(chunks // 2):
                y = x[p * ROWS : (p + 1) * ROWS]
                z = pltpu.roll(y, dim, 1)
                out += [jnp.where(even, y, z)[:, :dim], swap(jnp.where(even, z, y))[:, :dim]]
            o_ref[b] = jnp.concatenate(out, 0).astype(o_ref.dtype)
    all_but_one(parts.at[pl.ds(0, n - 1)], out_sem, in_sem.at[0]).wait_send()


def solution(mesh):
    n = mesh.shape["sp"]

    def step(q, k, v):
        batch, tokens, heads, dim = k.shape
        k, v = (x.transpose(0, 2, 3, 1).reshape(batch, heads * dim, tokens) for x in (k, v))
        chunks = heads // ROWS
        runs, segments = len(spans(batch, (2, 4))), len(spans(batch, (2, 3, 4)))
        hbm = pl.BlockSpec(memory_space=pl.ANY)
        dma = pltpu.SemaphoreType.DMA
        return pl.pallas_call(
            functools.partial(kernel, n),
            out_shape=jax.ShapeDtypeStruct(q.shape, q.dtype),
            in_specs=[hbm] * 3,
            out_specs=pl.BlockSpec(memory_space=pltpu.VMEM),
            scratch_shapes=[
                pltpu.VMEM(q.shape, q.dtype),
                pltpu.VMEM((SLOTS, heads * dim, tokens), k.dtype),
                pltpu.VMEM((SLOTS, heads * dim, tokens), v.dtype),
                pltpu.VMEM((LEAD + 1, chunks, ROWS, tokens), jnp.bfloat16),
                pltpu.VMEM((n, batch, heads // 2, 2 * dim), jnp.bfloat16),
                pltpu.VMEM((n, runs, ROWS, 128), jnp.float32),
                pltpu.VMEM((ROWS, 128), jnp.float32),
                dma,
                dma((SLOTS,)),
                dma((SLOTS,)),
                dma,
                dma((runs,)),
                dma,
                dma((segments - (batch - TAIL) // SOME + 1,)),
            ],
            compiler_params=pltpu.CompilerParams(collective_id=0, has_side_effects=True, vmem_limit_bytes=56114023),
            cost_estimate=pl.CostEstimate(flops=4 * k.size, bytes_accessed=4 * k.size, transcendentals=batch * heads * tokens),
        )(q, k, v)

    return jax.shard_map(
        step,
        mesh=mesh,
        in_specs=(P("dp", None, None), P("dp", "sp", None, None), P("dp", "sp", None, None)),
        out_specs=P("dp", None, None),
        check_vma=False,
    )
```
